32 devices in a mesh: stage: 2 (over x), model: 4 (over z), data: 4 (over y, core).
Axes of the slice: x: 2, y: 2, z: 4, core: 2. Of those that a mesh axis runs over, the one named last changes fastest.
Arguments:
- w_fc1: float32 [32, 1536, 1024], P('stage', 'data', 'model'), parts along dimension 0
- m_fc1: float32 [32, 1536, 1024], P('stage', 'data', 'model'), parts along dimension 0
- g_fc1: bfloat16 [32, 1536, 1024], P('stage', 'data', 'model'), parts along dimension 0
- w_fc2: float32 [32, 1536, 512], P('stage', 'data', 'model'), parts along dimension 0
- m_fc2: float32 [32, 1536, 512], P('stage', 'data', 'model'), parts along dimension 0
- g_fc2: bfloat16 [32, 1536, 512], P('stage', 'data', 'model'), parts along dimension 0
Outputs:
- output 1: float32 [32, 1536, 1024], P('stage', 'data', 'model'), parts along dimension 0
- output 2: float32 [32, 1536, 1024], P('stage', 'data', 'model'), parts along dimension 0
- output 3: float32 [32, 1536, 512], P('stage', 'data', 'model'), parts along dimension 0
- output 4: float32 [32, 1536, 512], P('stage', 'data', 'model'), parts along dimension 0
There are 2 independent parts. The reference program is written for one: setup_inputs(seed, part) draws one part's arguments, and reference() takes and returns one part's arrays. A program takes and returns all parts, laid end to end along the dimension named above; each array names one.
All inputs are finite; a program needn't handle non-finite values.
Results may differ from the reference program's by a relative error of at most 0.0082908.
Values are sent between devices in bfloat16 or wider.
A program may use at most 1 GiB of HBM per device.

```python
import math
import jax
import jax.numpy as jnp
from jax import lax

HIDDEN = 1536
EXPERT_FFN = 512
EXPERTS = 16
NS_STEPS = 5
LOW_RANK = 4

NS_COEF_A = 3.4445
NS_COEF_B = -4.7750
NS_COEF_C = 2.0315
MOMENTUM = 0.95
LEARN_RATE = 0.04
DECAY = 0.2
NORM_EPS = 1e-7


def draw_state(key, cols):
    key_noise, key_left, key_right, key_scale = jax.random.split(key, 4)
    noise = jax.random.normal(key_noise, (EXPERTS, HIDDEN, cols), jnp.float32)
    left = jax.random.normal(key_left, (EXPERTS, HIDDEN, LOW_RANK), jnp.float32)
    right = jax.random.normal(key_right, (EXPERTS, LOW_RANK, cols), jnp.float32)
    shared = jnp.einsum('emr,ern->emn', left, right) / math.sqrt(LOW_RANK)
    row_scale = jax.random.uniform(key_scale, (EXPERTS, HIDDEN, 1), jnp.float32, 0.5, 1.5)
    return row_scale * (noise + shared) * math.sqrt(0.5)


def setup_inputs(seed: int = 0, part: int = 0) -> dict:
    base = jax.random.fold_in(jax.random.key(seed), part)
    keys = jax.random.split(base, 6)
    fc1_cols = 2 * EXPERT_FFN
    w_scale = HIDDEN ** -0.5
    return {
        'w_fc1': jax.random.normal(keys[0], (EXPERTS, HIDDEN, fc1_cols), jnp.float32) * w_scale,
        'm_fc1': draw_state(keys[1], fc1_cols),
        'g_fc1': draw_state(keys[2], fc1_cols).astype(jnp.bfloat16),
        'w_fc2': jax.random.normal(keys[3], (EXPERTS, HIDDEN, EXPERT_FFN), jnp.float32) * w_scale,
        'm_fc2': draw_state(keys[4], EXPERT_FFN),
        'g_fc2': draw_state(keys[5], EXPERT_FFN).astype(jnp.bfloat16),
    }


def orthogonalize(momentum):
    row_count, col_count = momentum.shape
    norm_val = jnp.sqrt(jnp.sum(momentum * momentum))
    x_mat = (momentum.astype(jnp.bfloat16).astype(jnp.float32) / (norm_val + NORM_EPS)).astype(jnp.bfloat16)
    if row_count > col_count:
        x_mat = x_mat.T
    for ns_step in range(NS_STEPS):
        gram_mat = jnp.dot(x_mat, x_mat.T, preferred_element_type=jnp.float32).astype(jnp.bfloat16)
        gram_sq = jnp.dot(gram_mat, gram_mat, preferred_element_type=jnp.float32)
        poly_mat = (NS_COEF_B * gram_mat.astype(jnp.float32) + NS_COEF_C * gram_sq).astype(jnp.bfloat16)
        update_term = jnp.dot(poly_mat, x_mat, preferred_element_type=jnp.float32)
        x_mat = (NS_COEF_A * x_mat.astype(jnp.float32) + update_term).astype(jnp.bfloat16)
    if row_count > col_count:
        x_mat = x_mat.T
    return x_mat.astype(jnp.float32) * (0.2 * math.sqrt(max(row_count, col_count)))


def update_stack(weights, momentum, gradient):
    new_mom = MOMENTUM * momentum + gradient.astype(jnp.float32)
    ortho = lax.map(orthogonalize, new_mom)
    new_w = weights - LEARN_RATE * (ortho + DECAY * weights)
    return new_w, new_mom


def reference(w_fc1, m_fc1, g_fc1, w_fc2, m_fc2, g_fc2):
    new_w1, new_m1 = update_stack(w_fc1, m_fc1, g_fc1)
    new_w2, new_m2 = update_stack(w_fc2, m_fc2, g_fc2)
    return (new_w1, new_m1, new_w2, new_m2)
```

```python
import functools
import math
import jax
import jax.numpy as jnp
from jax import lax
from jax.experimental import pallas as pl
from jax.experimental.pallas import tpu as pltpu
from jax.sharding import PartitionSpec as P

NS_STEPS = 5
NS_COEF_A = 3.4445
NS_COEF_B = -4.7750
NS_COEF_C = 2.0315
MOMENTUM = 0.95
LEARN_RATE = 0.04
DECAY = 0.2
NORM_EPS = 1e-7

F32 = jnp.float32
BF16 = jnp.bfloat16
MESH = pl.DeviceIdType.MESH
TILE = 256


def flip(bit, offset):
    return bit + offset - 2 * bit * offset


def xor2(value, offset):
    high = flip(lax.div(value, 2), lax.div(offset, 2))
    low = flip(lax.rem(value, 2), lax.rem(offset, 2))
    return high * 2 + low


def fold_squares(mom):
    sq = mom * mom
    rows, cols = sq.shape
    acc = jnp.sum(sq.reshape(rows // 8, 8, cols), axis=0)
    out = acc[:, :128]
    for col in range(128, cols, 128):
        out = out + acc[:, col:col + 128]
    return out


def momentum_kernel(m1_ref, g1_ref, m2_ref, g2_ref, nm1_ref, b1_ref, nm2_ref, b2_ref, sq_ref):
    for slot, (m_ref, g_ref, nm_ref, b_ref) in enumerate(
            ((m1_ref, g1_ref, nm1_ref, b1_ref), (m2_ref, g2_ref, nm2_ref, b2_ref))):
        mom = MOMENTUM * m_ref[0] + g_ref[0].astype(F32)
        nm_ref[0] = mom
        b_ref[0] = mom.astype(BF16)
        sq_ref[0, slot * 8:slot * 8 + 8, :] = fold_squares(mom)


def momentum_step(m1, g1, m2, g2):
    experts = m1.shape[0]

    def spec(arr):
        return pl.BlockSpec((1,) + arr.shape[1:], lambda e: (e, 0, 0))
    sq_shape = jax.ShapeDtypeStruct((experts, 16, 128), F32)
    outs = (jax.ShapeDtypeStruct(m1.shape, F32), jax.ShapeDtypeStruct(m1.shape, BF16),
            jax.ShapeDtypeStruct(m2.shape, F32), jax.ShapeDtypeStruct(m2.shape, BF16), sq_shape)
    return pl.pallas_call(
        momentum_kernel, out_shape=outs, grid=(experts,),
        in_specs=[spec(m1), spec(g1), spec(m2), spec(g2)],
        out_specs=tuple(spec(o) for o in outs),
        name='momentum')(m1, g1, m2, g2)


def dot_tn(lhs, rhs):
    return lax.dot_general(lhs, rhs, (((0,), (0,)), ((), ())), preferred_element_type=F32)


def gram_and_poly(x, gram, poly):
    size = gram.shape[0]
    for blk in range(size // TILE):
        lo, hi = blk * TILE, (blk + 1) * TILE
        val = dot_tn(x[:, lo:hi], x[:, :hi]).astype(BF16)
        gram[lo:hi, :hi] = val
        if blk:
            gram[:lo, lo:hi] = val[:, :lo].T
    for blk in range(size // TILE):
        lo, hi = blk * TILE, (blk + 1) * TILE
        sq = jnp.dot(gram[lo:hi, :], gram[:, :hi], preferred_element_type=F32)
        val = (NS_COEF_B * gram[lo:hi, :hi].astype(F32) + NS_COEF_C * sq).astype(BF16)
        poly[lo:hi, :hi] = val
        if blk:
            poly[:lo, lo:hi] = val[:, :lo].T


def update_rows(x, poly, rows):
    old = x[rows, :]
    term = jnp.dot(old, poly[...], preferred_element_type=F32)
    x[rows, :] = (NS_COEF_A * old.astype(F32) + term).astype(BF16)


def newton_schulz(x, gram, poly, block_rows, last_rows):
    blocks = x.shape[0] // block_rows

    def one_block(i, carry):
        update_rows(x, poly, pl.ds(pl.multiple_of(i * block_rows, block_rows), block_rows))
        return carry

    def one_step(step, carry):
        gram_and_poly(x, gram, poly)

        @pl.when(step < NS_STEPS - 1)
        def _():
            lax.fori_loop(0, blocks, one_block, 0)
        return carry
    lax.fori_loop(0, NS_STEPS, one_step, 0)
    last_rows()


def exchange_kernel(b1_ref, b2_ref, sq_ref, o1_ref, o2_ref,
                    x1, x2, gram1, poly1, gram2, poly2, sq_in,
                    in_send, in_recv, sq_send, sq_recv, out_send, out_recv):
    data = lax.axis_index('data')
    model = lax.axis_index('model')
    me = data * 4 + model
    rows = b1_ref.shape[1]
    cols1, cols2 = b1_ref.shape[2], b2_ref.shape[2]

    def peer(slot):
        return xor2(data, lax.rem(slot, 4)), xor2(model, lax.div(slot, 4))

    def each_peer(action):
        def body(slot, carry):
            action(slot, *peer(slot))
            return carry
        lax.fori_loop(1, 16, body, 0)

    def row_slice(index):
        return pl.ds(pl.multiple_of(index * rows, rows), rows)

    def col_slice(index, cols):
        return pl.ds(pl.multiple_of(index * cols, cols), cols)

    def remote(source, target, send, recv, to_data, to_model):
        return pltpu.make_async_remote_copy(
            src_ref=source, dst_ref=target, send_sem=send, recv_sem=recv,
            device_id={'data': to_data, 'model': to_model}, device_id_type=MESH)

    barrier = pltpu.get_barrier_semaphore()

    def greet(slot, to_data, to_model):
        pl.semaphore_signal(barrier, inc=1, device_id={'data': to_data, 'model': to_model}, device_id_type=MESH)
    each_peer(greet)
    pl.semaphore_wait(barrier, 15)

    arrays = ((b1_ref, x1, o1_ref, cols1), (b2_ref, x2, o2_ref, cols2))

    def copy_sq(slot, to_data, to_model):
        return remote(sq_ref.at[to_data * 4 + to_model], sq_in.at[slot], sq_send.at[slot], sq_recv.at[slot],
                      to_data, to_model)

    def copy_in(which, slot, to_data, to_model):
        src, dst, _, cols = arrays[which]
        return remote(src.at[to_data * 4 + to_model], dst.at[row_slice(data), col_slice(model, cols)],
                      in_send.at[which, slot], in_recv.at[which, slot], to_data, to_model)

    def own_in(which):
        src, dst, _, cols = arrays[which]
        return pltpu.make_async_copy(src.at[me], dst.at[row_slice(data), col_slice(model, cols)],
                                     in_recv.at[which, 0])

    def copy_out(which, slot, to_data, to_model):
        _, src, dst, cols = arrays[which]
        return remote(src.at[row_slice(to_data), col_slice(to_model, cols)], dst.at[me],
                      out_send.at[which, slot], out_recv.at[which, slot], to_data, to_model)

    def own_out(which):
        _, src, dst, cols = arrays[which]
        return pltpu.make_async_copy(src.at[row_slice(data), col_slice(model, cols)], dst.at[me],
                                     out_recv.at[which, 0])

    each_peer(lambda *at: copy_sq(*at).start())
    for which in (1, 0):
        own_in(which).start()
        each_peer(lambda *at: copy_in(which, *at).start())

    sq_in[0] = sq_ref[me]
    each_peer(lambda *at: copy_sq(*at).wait())
    total = jnp.sum(sq_in[...], axis=0)
    norm1 = jnp.sqrt(jnp.sum(total[:8], keepdims=True)) + NORM_EPS
    norm2 = jnp.sqrt(jnp.sum(total[8:], keepdims=True)) + NORM_EPS

    def receive(which, norm):
        _, x, _, cols = arrays[which]

        def scale(from_data, from_model):
            at = (row_slice(from_data), col_slice(from_model, cols))
            x[at] = (x[at].astype(F32) / norm).astype(BF16)

        def take(slot, from_data, from_model):
            copy_in(which, slot, from_data, from_model).wait_recv()
            scale(from_data, from_model)
        own_in(which).wait()
        scale(data, model)
        each_peer(take)

    receive(1, norm2)

    def finish2():
        def body(i, carry):
            update_rows(x2, poly2, row_slice(i))
            return carry
        lax.fori_loop(0, 4, body, 0)
    newton_schulz(x2, gram2, poly2, rows, finish2)

    receive(0, norm1)
    own_out(1).start()
    each_peer(lambda *at: copy_out(1, *at).start())

    def finish1():
        update_rows(x1, poly1, row_slice(data))
        own_out(0).start()
        for dz in (1, 2, 3):
            copy_out(0, dz * 4, *peer(dz * 4)).start()

        def body(dd, carry):
            update_rows(x1, poly1, row_slice(xor2(data, dd)))
            for dz in range(4):
                slot = dz * 4 + dd
                copy_out(0, slot, *peer(slot)).start()
            return carry
        lax.fori_loop(1, 4, body, 0)
    newton_schulz(x1, gram1, poly1, rows, finish1)

    for which in (1, 0):
        each_peer(lambda *at: copy_in(which, *at).wait_send())
    for which in (1, 0):
        own_out(which).wait()
        each_peer(lambda *at: copy_out(which, *at).wait())


def exchange_step(b1, b2, sq):
    rows, cols1, cols2 = b1.shape[1], b1.shape[2], b2.shape[2]
    full_rows, size1, size2 = rows * 4, cols1 * 4, cols2 * 4
    any_spec = pl.BlockSpec(memory_space=pl.ANY)
    vmem_spec = pl.BlockSpec(memory_space=pltpu.VMEM)
    return pl.pallas_call(
        exchange_kernel,
        out_shape=(jax.ShapeDtypeStruct(b1.shape, BF16), jax.ShapeDtypeStruct(b2.shape, BF16)),
        in_specs=[any_spec, any_spec, vmem_spec],
        out_specs=(any_spec, any_spec),
        scratch_shapes=[
            pltpu.VMEM((full_rows, size1), BF16), pltpu.VMEM((full_rows, size2), BF16),
            pltpu.VMEM((size1, size1), BF16), pltpu.VMEM((size1, size1), BF16),
            pltpu.VMEM((size2, size2), BF16), pltpu.VMEM((size2, size2), BF16),
            pltpu.VMEM((16, 16, 128), F32),
            pltpu.SemaphoreType.DMA((2, 16)), pltpu.SemaphoreType.DMA((2, 16)),
            pltpu.SemaphoreType.DMA((16,)), pltpu.SemaphoreType.DMA((16,)),
            pltpu.SemaphoreType.DMA((2, 16)), pltpu.SemaphoreType.DMA((2, 16)),
        ],
        compiler_params=pltpu.CompilerParams(
            collective_id=0, has_side_effects=True, vmem_limit_bytes=48 << 20),
        name='exchange')(b1, b2, sq)


def weight_step(w, ortho, row_count, col_count):
    scale = 0.2 * math.sqrt(max(row_count, col_count))
    return w - LEARN_RATE * (ortho.astype(F32) * scale + DECAY * w)


def solution(mesh):
    data_size = mesh.shape['data']
    model_size = mesh.shape['model']
    block_spec = P('stage', 'data', 'model')

    def local_step(w1, m1, g1, w2, m2, g2):
        new_m1, b1, new_m2, b2, sq = momentum_step(m1, g1, m2, g2)
        x1, x2 = exchange_step(b1, b2, sq)
        rows = m1.shape[1] * data_size
        new_w1 = weight_step(w1, x1, rows, m1.shape[2] * model_size)
        new_w2 = weight_step(w2, x2, rows, m2.shape[2] * model_size)
        return new_w1, new_m1, new_w2, new_m2

    return jax.shard_map(local_step, mesh=mesh, in_specs=(block_spec,) * 6, out_specs=(block_spec,) * 4, check_vma=False)
```

```python
import math
import jax
import jax.numpy as jnp
from jax import lax
from jax.experimental import pallas as pl
from jax.experimental.pallas import tpu as pltpu
from jax.sharding import PartitionSpec as P

NS_STEPS = 5
NS_COEF_A = 3.4445
NS_COEF_B = -4.7750
NS_COEF_C = 2.0315
MOMENTUM = 0.95
LEARN_RATE = 0.04
DECAY = 0.2
NORM_EPS = 1e-7

F32 = jnp.float32
BF16 = jnp.bfloat16
MESH = pl.DeviceIdType.MESH
TILE = 256
RETURN_STEP = 3
DZ_FAST = True
SWAP = True


def flip(bit, offset):
    return bit + offset - 2 * bit * offset


def xor2(value, offset):
    high = flip(lax.div(value, 2), lax.div(offset, 2))
    low = flip(lax.rem(value, 2), lax.rem(offset, 2))
    return high * 2 + low


def fold_squares(mom):
    sq = mom * mom
    rows, cols = sq.shape
    acc = jnp.sum(sq.reshape(rows // 8, 8, cols), axis=0)
    out = acc[:, :128]
    for col in range(128, cols, 128):
        out = out + acc[:, col:col + 128]
    return out


def dot_tn(lhs, rhs):
    return lax.dot_general(lhs, rhs, (((0,), (0,)), ((), ())), preferred_element_type=F32)


def gram_and_poly(x, gram, poly):
    size = gram.shape[0]
    for blk in range(size // TILE):
        lo, hi = blk * TILE, (blk + 1) * TILE
        val = dot_tn(x[:, lo:hi], x[:, :hi]).astype(BF16)
        gram[lo:hi, :hi] = val
        if blk:
            gram[:lo, lo:hi] = val[:, :lo].T
    for blk in range(size // TILE):
        lo, hi = blk * TILE, (blk + 1) * TILE
        sq = jnp.dot(gram[lo:hi, :], gram[:, :hi], preferred_element_type=F32)
        val = (NS_COEF_B * gram[lo:hi, :hi].astype(F32) + NS_COEF_C * sq).astype(BF16)
        poly[lo:hi, :hi] = val
        if blk:
            poly[:lo, lo:hi] = val[:, :lo].T


def update_rows(x, poly, rows):
    old = x[rows, :]
    term = jnp.dot(old, poly[...], preferred_element_type=F32)
    x[rows, :] = (NS_COEF_A * old.astype(F32) + term).astype(BF16)


def newton_schulz(x, gram, poly, block_rows, before_step, last_rows):
    blocks = x.shape[0] // block_rows

    def one_block(i, carry):
        update_rows(x, poly, pl.ds(pl.multiple_of(i * block_rows, block_rows), block_rows))
        return carry

    def one_step(step, carry):
        before_step(step)
        gram_and_poly(x, gram, poly)

        @pl.when(step < NS_STEPS - 1)
        def _():
            lax.fori_loop(0, blocks, one_block, 0)
        return carry
    lax.fori_loop(0, NS_STEPS, one_step, 0)
    last_rows()


def muon_kernel(w1_ref, m1_ref, g1_ref, w2_ref, m2_ref, g2_ref,
                nw1, nm1, nw2, nm2,
                b1, b2, x1, x2, o1, o2, gram1, poly1, gram2, poly2, sq_out, sq_in,
                m_load, g_load, w_load, in_send, in_recv, sq_send, sq_recv, out_send, out_recv):
    data = lax.axis_index('data')
    model = lax.axis_index('model')
    core = lax.rem(data, 2)
    me = data * 4 + model
    rows = b1.shape[1]
    stacks = ((m1_ref, g1_ref, w1_ref, nw1, nm1, b1, x1, o1, b1.shape[2]),
              (m2_ref, g2_ref, w2_ref, nw2, nm2, b2, x2, o2, b2.shape[2]))

    def peer(slot):
        return xor2(data, lax.rem(slot, 4)), xor2(model, lax.div(slot, 4))

    def expert_of(slot):
        to_data, to_model = peer(slot)
        return to_data * 4 + to_model

    def loop(lo, hi, action):
        def body(i, carry):
            action(i)
            return carry
        lax.fori_loop(lo, hi, body, 0)

    inner = flip(lax.rem(model, 2), lax.div(model, 2))

    def slot_of(dz, dd):
        high = lax.div(dz, 2)
        if SWAP:
            dz = high * 2 + flip(lax.rem(dz, 2), high * inner)
        return dz * 4 + dd

    def slot_at(i):
        if DZ_FAST:
            return slot_of(lax.rem(i, 4), lax.div(i, 4))
        return slot_of(lax.div(i, 4), lax.rem(i, 4))

    def core_slots(target_core, action):
        low = flip(core, target_core)

        def at(j):
            if DZ_FAST:
                return slot_of(lax.rem(j, 4), lax.div(j, 4) * 2 + low)
            return slot_of(lax.div(j, 2), lax.rem(j, 2) * 2 + low)
        loop(0, 8, lambda j: action(at(j)))

    def row_slice(index):
        return pl.ds(pl.multiple_of(index * rows, rows), rows)

    def col_slice(index, cols):
        return pl.ds(pl.multiple_of(index * cols, cols), cols)

    def remote(source, target, send, recv, slot):
        to_data, to_model = peer(slot)
        return pltpu.make_async_remote_copy(
            src_ref=source, dst_ref=target, send_sem=send, recv_sem=recv,
            device_id={'data': to_data, 'model': to_model}, device_id_type=MESH)

    def load_m(which, slot):
        e = expert_of(slot)
        return pltpu.make_async_copy(stacks[which][0].at[e], stacks[which][4].at[e], m_load.at[which, slot])

    def load_g(which, slot):
        e = expert_of(slot)
        return pltpu.make_async_copy(stacks[which][1].at[e], stacks[which][5].at[e], g_load.at[which, slot])

    def load_w(which):
        return pltpu.make_async_copy(stacks[which][2], stacks[which][3], w_load.at[which])

    def copy_sq(which, slot):
        return remote(sq_out.at[which, slot], sq_in.at[which, slot],
                      sq_send.at[which, slot], sq_recv.at[which, slot], slot)

    def copy_in(which, slot):
        src, dst, cols = stacks[which][5], stacks[which][6], stacks[which][8]
        return remote(src.at[expert_of(slot)], dst.at[row_slice(data), col_slice(model, cols)],
                      in_send.at[which, slot], in_recv.at[which, slot], slot)

    def copy_out(which, slot):
        src, dst, cols = stacks[which][6], stacks[which][7], stacks[which][8]
        to_data, to_model = peer(slot)
        return remote(src.at[row_slice(to_data), col_slice(to_model, cols)], dst.at[me],
                      out_send.at[which, slot], out_recv.at[which, slot], slot)

    def momentum(which, slot):
        nm, blocks = stacks[which][4], stacks[which][5]
        e = expert_of(slot)
        load_m(which, slot).wait()
        load_g(which, slot).wait()
        mom = MOMENTUM * nm[e] + blocks[e].astype(F32)
        nm[e] = mom
        blocks[e] = mom.astype(BF16)
        sq_out[which, slot] = fold_squares(mom)

    def norm_of(which):
        loop(1, 16, lambda slot: copy_sq(which, slot).wait_recv())
        total = jnp.sum(sq_in[which], axis=0)
        return jnp.sqrt(jnp.sum(total, keepdims=True)) + NORM_EPS

    def receive(which):
        blocks, x, cols = stacks[which][5], stacks[which][6], stacks[which][8]
        sq_in[which, 0] = sq_out[which, 0]
        norm = norm_of(which)
        own = (row_slice(data), col_slice(model, cols))
        x[own] = (blocks[me].astype(F32) / norm).astype(BF16)

        def take(slot):
            copy_in(which, slot).wait_recv()
            from_data, from_model = peer(slot)
            at = (row_slice(from_data), col_slice(from_model, cols))
            x[at] = (x[at].astype(F32) / norm).astype(BF16)
        loop(1, 16, take)

    def weight_step(which, e, ortho):
        new_w, x, cols = stacks[which][3], stacks[which][6], stacks[which][8]
        scale = 0.2 * math.sqrt(max(x.shape[0], x.shape[1]))
        old = new_w[e]
        new_w[e] = old - LEARN_RATE * (ortho.astype(F32) * scale + DECAY * old)

    def own_step(which):
        x, cols = stacks[which][6], stacks[which][8]
        weight_step(which, me, x[row_slice(data), col_slice(model, cols)])

    def peer_step(which, slot):
        copy_out(which, slot).wait_recv()
        e = expert_of(slot)
        weight_step(which, e, stacks[which][7][e])

    for which in (1, 0):
        def load(slot):
            load_m(which, slot).start()
            load_g(which, slot).start()
        if which:
            loop(1, 16, lambda i: load(slot_at(i)))
            load(0)
        else:
            loop(0, 16, load)
    load_w(1).start()
    load_w(0).start()

    barrier = pltpu.get_barrier_semaphore()

    def greet(slot):
        to_data, to_model = peer(slot)
        pl.semaphore_signal(barrier, inc=1, device_id={'data': to_data, 'model': to_model}, device_id_type=MESH)
    loop(1, 16, greet)
    pl.semaphore_wait(barrier, 15)

    def send2(slot):
        copy_sq(1, slot).start()
        copy_in(1, slot).start()

    def first(i):
        momentum(1, slot_at(i))

        @pl.when(i > 1)
        def _():
            send2(slot_at(i - 1))
    loop(1, 16, first)
    momentum(1, 0)
    send2(slot_at(15))

    loop(0, 16, lambda i: momentum(0, 15 - i))
    loop(1, 16, lambda slot: copy_sq(0, slot).start())

    def send1(slot):
        @pl.when(slot > 0)
        def _():
            copy_in(0, slot).start()
    core_slots(0, send1)
    core_slots(1, send1)

    receive(1)

    def finish2():
        loop(0, 4, lambda i: update_rows(x2, poly2, row_slice(i)))
    newton_schulz(x2, gram2, poly2, rows, lambda step: None, finish2)

    receive(0)
    return_step = (1 - core) * RETURN_STEP

    def before_step(step):
        @pl.when(step == return_step)
        def _():
            loop(1, 16, lambda i: copy_out(1, slot_at(i)).start())

    def finish1():
        update_rows(x1, poly1, row_slice(data))

        def body(dd):
            update_rows(x1, poly1, row_slice(xor2(data, dd)))
            for dz in range(4):
                slot = slot_of(dz, dd - 1)

                @pl.when(slot > 0)
                def _():
                    copy_out(0, slot).start()
        loop(1, 4, body)
        load_w(1).wait()
        own_step(1)
        for dz in range(4):
            copy_out(0, slot_of(dz, 3)).start()
    newton_schulz(x1, gram1, poly1, rows, before_step, finish1)

    load_w(0).wait()
    own_step(0)
    loop(1, 16, lambda slot: peer_step(1, slot))
    for which in (1, 0):
        def sent(slot):
            copy_in(which, slot).wait_send()
            copy_sq(which, slot).wait_send()
        loop(1, 16, sent)
    for target_core in (0, 1):
        def take(slot):
            @pl.when(slot > 0)
            def _():
                peer_step(0, slot)
        core_slots(target_core, take)
    for which in (1, 0):
        loop(1, 16, lambda slot: copy_out(which, slot).wait_send())


def solution(mesh):
    block_spec = P('stage', 'data', 'model')

    def local_step(w1, m1, g1, w2, m2, g2):
        experts, rows, cols1 = m1.shape
        cols2 = m2.shape[2]
        full_rows, size1, size2 = rows * 4, cols1 * 4, cols2 * 4
        dma = pltpu.SemaphoreType.DMA
        scratch = [pltpu.VMEM(g1.shape, BF16), pltpu.VMEM(g2.shape, BF16),
                   pltpu.VMEM((full_rows, size1), BF16), pltpu.VMEM((full_rows, size2), BF16),
                   pltpu.VMEM(g1.shape, BF16), pltpu.VMEM(g2.shape, BF16),
                   pltpu.VMEM((size1, size1), BF16), pltpu.VMEM((size1, size1), BF16),
                   pltpu.VMEM((size2, size2), BF16), pltpu.VMEM((size2, size2), BF16),
                   pltpu.VMEM((2, 16, 8, 128), F32), pltpu.VMEM((2, 16, 8, 128), F32),
                   dma((2, 16)), dma((2, 16)), dma((2,))] + [dma((2, 16))] * 6
        return pl.pallas_call(
            muon_kernel,
            out_shape=tuple(pltpu.VMEM(a.shape, F32) for a in (w1, m1, w2, m2)),
            in_specs=[pl.BlockSpec(memory_space=pl.ANY)] * 6,
            out_specs=(pl.BlockSpec(memory_space=pltpu.VMEM),) * 4,
            scratch_shapes=scratch,
            compiler_params=pltpu.CompilerParams(
                collective_id=0, has_side_effects=True, vmem_limit_bytes=36 << 20),
            name='muon')(w1, m1, g1, w2, m2, g2)

    return jax.shard_map(local_step, mesh=mesh, in_specs=(block_spec,) * 6, out_specs=(block_spec,) * 4, check_vma=False)
```

```python
import math
import jax
import jax.numpy as jnp
from jax import lax
from jax.experimental import pallas as pl
from jax.experimental.pallas import tpu as pltpu
from jax.sharding import PartitionSpec as P

NS_STEPS = 5
NS_COEF_A = 3.4445
NS_COEF_B = -4.7750
NS_COEF_C = 2.0315
MOMENTUM = 0.95
LEARN_RATE = 0.04
DECAY = 0.2
NORM_EPS = 1e-7

F32 = jnp.float32
BF16 = jnp.bfloat16
MESH = pl.DeviceIdType.MESH
TILE = 256
DZ_FAST = True
SWAP = True


def flip(bit, offset):
    return bit + offset - 2 * bit * offset


def xor2(value, offset):
    high = flip(lax.div(value, 2), lax.div(offset, 2))
    low = flip(lax.rem(value, 2), lax.rem(offset, 2))
    return high * 2 + low


def fold_squares(mom):
    sq = mom * mom
    rows, cols = sq.shape
    acc = jnp.sum(sq.reshape(rows // 8, 8, cols), axis=0)
    out = acc[:, :128]
    for col in range(128, cols, 128):
        out = out + acc[:, col:col + 128]
    return out


def dot_tn(lhs, rhs):
    return lax.dot_general(lhs, rhs, (((0,), (0,)), ((), ())), preferred_element_type=F32)


def gram_and_poly(x, gram, poly):
    size = gram.shape[0]
    for blk in range(size // TILE):
        lo, hi = blk * TILE, (blk + 1) * TILE
        val = dot_tn(x[:, lo:hi], x[:, :hi]).astype(BF16)
        gram[lo:hi, :hi] = val
        if blk:
            gram[:lo, lo:hi] = val[:, :lo].T
    for blk in range(size // TILE):
        lo, hi = blk * TILE, (blk + 1) * TILE
        sq = jnp.dot(gram[lo:hi, :], gram[:, :hi], preferred_element_type=F32)
        val = (NS_COEF_B * gram[lo:hi, :hi].astype(F32) + NS_COEF_C * sq).astype(BF16)
        poly[lo:hi, :hi] = val
        if blk:
            poly[:lo, lo:hi] = val[:, :lo].T


def update_rows(x, poly, rows):
    old = x[rows, :]
    term = jnp.dot(old, poly[...], preferred_element_type=F32)
    x[rows, :] = (NS_COEF_A * old.astype(F32) + term).astype(BF16)


def newton_schulz(x, gram, poly, block_rows, last_rows):
    blocks = x.shape[0] // block_rows

    def one_block(i, carry):
        update_rows(x, poly, pl.ds(pl.multiple_of(i * block_rows, block_rows), block_rows))
        return carry

    def one_step(step, carry):
        gram_and_poly(x, gram, poly)

        @pl.when(step < NS_STEPS - 1)
        def _():
            lax.fori_loop(0, blocks, one_block, 0)
        return carry
    lax.fori_loop(0, NS_STEPS, one_step, 0)
    last_rows()


def muon_kernel(w1_ref, m1_ref, g1_ref, w2_ref, m2_ref, g2_ref,
                nw1, nm1, nw2, nm2,
                b1, b2, x1, x2, o1, o2, gram1, poly1, gram2, poly2, sq_out, sq_in,
                m_load, g_load, w_load, in_send, in_recv, sq_send, sq_recv, out_send, out_recv):
    data = lax.axis_index('data')
    model = lax.axis_index('model')
    core = lax.rem(data, 2)
    me = data * 4 + model
    rows = b1.shape[1]
    stacks = ((m1_ref, g1_ref, w1_ref, nw1, nm1, b1, x1, o1, b1.shape[2]),
              (m2_ref, g2_ref, w2_ref, nw2, nm2, b2, x2, o2, b2.shape[2]))

    def peer(slot):
        return xor2(data, lax.rem(slot, 4)), xor2(model, lax.div(slot, 4))

    def expert_of(slot):
        to_data, to_model = peer(slot)
        return to_data * 4 + to_model

    def loop(lo, hi, action):
        def body(i, carry):
            action(i)
            return carry
        lax.fori_loop(lo, hi, body, 0)

    inner = flip(lax.rem(model, 2), lax.div(model, 2))

    def slot_of(dz, dd):
        high = lax.div(dz, 2)
        if SWAP:
            dz = high * 2 + flip(lax.rem(dz, 2), high * inner)
        return dz * 4 + dd

    def slot_at(i):
        if DZ_FAST:
            return slot_of(lax.rem(i, 4), lax.div(i, 4))
        return slot_of(lax.div(i, 4), lax.rem(i, 4))

    def core_slots(target_core, action):
        low = flip(core, target_core)

        def at(j):
            if DZ_FAST:
                return slot_of(lax.rem(j + 2 * core, 4), lax.div(j, 4) * 2 + low)
            return slot_of(lax.div(j, 2), lax.rem(j, 2) * 2 + low)
        loop(0, 8, lambda j: action(at(j)))

    def row_slice(index):
        return pl.ds(pl.multiple_of(index * rows, rows), rows)

    def col_slice(index, cols):
        return pl.ds(pl.multiple_of(index * cols, cols), cols)

    def remote(source, target, send, recv, slot):
        to_data, to_model = peer(slot)
        return pltpu.make_async_remote_copy(
            src_ref=source, dst_ref=target, send_sem=send, recv_sem=recv,
            device_id={'data': to_data, 'model': to_model}, device_id_type=MESH)

    def load_m(which, slot):
        e = expert_of(slot)
        return pltpu.make_async_copy(stacks[which][0].at[e], stacks[which][4].at[e], m_load.at[which, slot])

    def load_g(which, slot):
        e = expert_of(slot)
        return pltpu.make_async_copy(stacks[which][1].at[e], stacks[which][5].at[e], g_load.at[which, slot])

    def load_w(which):
        return pltpu.make_async_copy(stacks[which][2], stacks[which][3], w_load.at[which])

    def copy_sq(which, slot):
        return remote(sq_out.at[which, slot], sq_in.at[which, slot],
                      sq_send.at[which, slot], sq_recv.at[which, slot], slot)

    def copy_in(which, slot):
        src, dst, cols = stacks[which][5], stacks[which][6], stacks[which][8]
        return remote(src.at[expert_of(slot)], dst.at[row_slice(data), col_slice(model, cols)],
                      in_send.at[which, slot], in_recv.at[which, slot], slot)

    def copy_out(which, slot):
        src, dst, cols = stacks[which][6], stacks[which][7], stacks[which][8]
        to_data, to_model = peer(slot)
        return remote(src.at[row_slice(to_data), col_slice(to_model, cols)], dst.at[me],
                      out_send.at[which, slot], out_recv.at[which, slot], slot)

    def momentum(which, slot):
        nm, blocks = stacks[which][4], stacks[which][5]
        e = expert_of(slot)
        load_m(which, slot).wait()
        load_g(which, slot).wait()
        mom = MOMENTUM * nm[e] + blocks[e].astype(F32)
        nm[e] = mom
        blocks[e] = mom.astype(BF16)
        sq_out[which, slot] = fold_squares(mom)

    def norm_of(which):
        loop(1, 16, lambda slot: copy_sq(which, slot).wait_recv())
        total = jnp.sum(sq_in[which], axis=0)
        return jnp.sqrt(jnp.sum(total, keepdims=True)) + NORM_EPS

    def receive(which):
        blocks, x, cols = stacks[which][5], stacks[which][6], stacks[which][8]
        sq_in[which, 0] = sq_out[which, 0]
        norm = norm_of(which)
        own = (row_slice(data), col_slice(model, cols))
        x[own] = (blocks[me].astype(F32) / norm).astype(BF16)

        def take(slot):
            copy_in(which, slot).wait_recv()
            from_data, from_model = peer(slot)
            at = (row_slice(from_data), col_slice(from_model, cols))
            x[at] = (x[at].astype(F32) / norm).astype(BF16)
        loop(1, 16, take)

    def weight_step(which, e, ortho):
        new_w, x, cols = stacks[which][3], stacks[which][6], stacks[which][8]
        scale = 0.2 * math.sqrt(max(x.shape[0], x.shape[1]))
        old = new_w[e]
        new_w[e] = old - LEARN_RATE * (ortho.astype(F32) * scale + DECAY * old)

    def own_step(which):
        x, cols = stacks[which][6], stacks[which][8]
        weight_step(which, me, x[row_slice(data), col_slice(model, cols)])

    def peer_step(which, slot):
        copy_out(which, slot).wait_recv()
        e = expert_of(slot)
        weight_step(which, e, stacks[which][7][e])

    for which in (1, 0):
        def load(slot):
            load_m(which, slot).start()
            load_g(which, slot).start()
        if which:
            loop(1, 16, lambda i: load(slot_at(i)))
            load(0)
        else:
            loop(0, 16, load)
    load_w(1).start()
    load_w(0).start()

    barrier = pltpu.get_barrier_semaphore()

    def greet(slot):
        to_data, to_model = peer(slot)
        pl.semaphore_signal(barrier, inc=1, device_id={'data': to_data, 'model': to_model}, device_id_type=MESH)
    loop(1, 16, greet)
    pl.semaphore_wait(barrier, 15)

    def send2(slot):
        copy_sq(1, slot).start()
        copy_in(1, slot).start()

    def first(i):
        momentum(1, slot_at(i))

        @pl.when(i > 1)
        def _():
            send2(slot_at(i - 1))
    loop(1, 16, first)
    momentum(1, 0)
    send2(slot_at(15))

    loop(0, 16, lambda i: momentum(0, 15 - i))
    loop(1, 16, lambda slot: copy_sq(0, slot).start())

    def send1(slot):
        @pl.when(slot > 0)
        def _():
            copy_in(0, slot).start()
    core_slots(0, send1)
    core_slots(1, send1)

    receive(1)

    def finish2():
        loop(0, 4, lambda i: update_rows(x2, poly2, row_slice(i)))
    newton_schulz(x2, gram2, poly2, rows, finish2)
    loop(1, 16, lambda i: copy_out(1, slot_at(i)).start())

    receive(0)
    def finish1():
        update_rows(x1, poly1, row_slice(data))

        def body(dd):
            update_rows(x1, poly1, row_slice(xor2(data, dd)))
            for dz in range(4):
                slot = slot_of(lax.rem(dz + 2 * core, 4), dd - 1)

                @pl.when(slot > 0)
                def _():
                    copy_out(0, slot).start()
        loop(1, 4, body)
        load_w(1).wait()
        own_step(1)
        for dz in range(4):
            copy_out(0, slot_of(lax.rem(dz + 2 * core, 4), 3)).start()
    newton_schulz(x1, gram1, poly1, rows, finish1)

    load_w(0).wait()
    own_step(0)
    loop(1, 16, lambda slot: peer_step(1, slot))
    for which in (1, 0):
        def sent(slot):
            copy_in(which, slot).wait_send()
            copy_sq(which, slot).wait_send()
        loop(1, 16, sent)
    for target_core in (0, 1):
        def take(slot):
            @pl.when(slot > 0)
            def _():
                peer_step(0, slot)
        core_slots(target_core, take)
    for which in (1, 0):
        loop(1, 16, lambda slot: copy_out(which, slot).wait_send())


def store_kernel(*refs):
    sources, targets, sems = refs[:4], refs[4:8], refs[8]
    step = 4
    copies = []
    for which in range(4):
        for part in range(16 // step):
            at = pl.ds(part * step, step)
            copies.append(pltpu.make_async_copy(
                sources[which].at[at], targets[which].at[at], sems.at[which, part]))
    for copy in copies:
        copy.start()
    for copy in copies:
        copy.wait()


def store(arrays):
    return pl.pallas_call(
        store_kernel,
        out_shape=tuple(jax.ShapeDtypeStruct(a.shape, a.dtype) for a in arrays),
        in_specs=[pl.BlockSpec(memory_space=pltpu.VMEM)] * 4,
        out_specs=(pl.BlockSpec(memory_space=pl.ANY),) * 4,
        scratch_shapes=[pltpu.SemaphoreType.DMA((4, 4))],
        compiler_params=pltpu.CompilerParams(vmem_limit_bytes=1 << 20),
        name='store')(*(pltpu.with_memory_space_constraint(a, pltpu.VMEM) for a in arrays))


def solution(mesh):
    block_spec = P('stage', 'data', 'model')

    def local_step(w1, m1, g1, w2, m2, g2):
        experts, rows, cols1 = m1.shape
        cols2 = m2.shape[2]
        full_rows, size1, size2 = rows * 4, cols1 * 4, cols2 * 4
        dma = pltpu.SemaphoreType.DMA
        scratch = [pltpu.VMEM(g1.shape, BF16), pltpu.VMEM(g2.shape, BF16),
                   pltpu.VMEM((full_rows, size1), BF16), pltpu.VMEM((full_rows, size2), BF16),
                   pltpu.VMEM(g1.shape, BF16), pltpu.VMEM(g2.shape, BF16),
                   pltpu.VMEM((size1, size1), BF16), pltpu.VMEM((size1, size1), BF16),
                   pltpu.VMEM((size2, size2), BF16), pltpu.VMEM((size2, size2), BF16),
                   pltpu.VMEM((2, 16, 8, 128), F32), pltpu.VMEM((2, 16, 8, 128), F32),
                   dma((2, 16)), dma((2, 16)), dma((2,))] + [dma((2, 16))] * 6
        return store(pl.pallas_call(
            muon_kernel,
            out_shape=tuple(pltpu.VMEM(a.shape, F32) for a in (w1, m1, w2, m2)),
            in_specs=[pl.BlockSpec(memory_space=pl.ANY)] * 6,
            out_specs=(pl.BlockSpec(memory_space=pltpu.VMEM),) * 4,
            scratch_shapes=scratch,
            compiler_params=pltpu.CompilerParams(
                collective_id=0, has_side_effects=True, vmem_limit_bytes=36 << 20),
            name='muon')(w1, m1, g1, w2, m2, g2))

    return jax.shard_map(local_step, mesh=mesh, in_specs=(block_spec,) * 6, out_specs=(block_spec,) * 4, check_vma=False)
```

```python
import math
import jax
import jax.numpy as jnp
from jax import lax
from jax.experimental import pallas as pl
from jax.experimental.pallas import tpu as pltpu
from jax.sharding import PartitionSpec as P

NS_STEPS = 5
NS_COEF_A = 3.4445
NS_COEF_B = -4.7750
NS_COEF_C = 2.0315
MOMENTUM = 0.95
LEARN_RATE = 0.04
DECAY = 0.2
NORM_EPS = 1e-7

F32 = jnp.float32
BF16 = jnp.bfloat16
MESH = pl.DeviceIdType.MESH
TILE = 256
DZ_FAST = True
SWAP = True


def flip(bit, offset):
    return bit + offset - 2 * bit * offset


def xor2(value, offset):
    high = flip(lax.div(value, 2), lax.div(offset, 2))
    low = flip(lax.rem(value, 2), lax.rem(offset, 2))
    return high * 2 + low


def fold_squares(mom):
    sq = mom * mom
    rows, cols = sq.shape
    acc = jnp.sum(sq.reshape(rows // 8, 8, cols), axis=0)
    out = acc[:, :128]
    for col in range(128, cols, 128):
        out = out + acc[:, col:col + 128]
    return out


def dot_tn(lhs, rhs):
    return lax.dot_general(lhs, rhs, (((0,), (0,)), ((), ())), preferred_element_type=F32)


def gram_and_poly(x, gram, poly):
    size = gram.shape[0]
    for blk in range(size // TILE):
        lo, hi = blk * TILE, (blk + 1) * TILE
        val = dot_tn(x[:, lo:hi], x[:, :hi]).astype(BF16)
        gram[lo:hi, :hi] = val
        if blk:
            gram[:lo, lo:hi] = val[:, :lo].T
    for blk in range(size // TILE):
        lo, hi = blk * TILE, (blk + 1) * TILE
        sq = jnp.dot(gram[lo:hi, :], gram[:, :hi], preferred_element_type=F32)
        val = (NS_COEF_B * gram[lo:hi, :hi].astype(F32) + NS_COEF_C * sq).astype(BF16)
        poly[lo:hi, :hi] = val
        if blk:
            poly[:lo, lo:hi] = val[:, :lo].T


def update_rows(x, poly, rows):
    old = x[rows, :]
    term = jnp.dot(old, poly[...], preferred_element_type=F32)
    x[rows, :] = (NS_COEF_A * old.astype(F32) + term).astype(BF16)


def newton_schulz(x, gram, poly, block_rows, last_rows):
    blocks = x.shape[0] // block_rows

    def one_block(i, carry):
        update_rows(x, poly, pl.ds(pl.multiple_of(i * block_rows, block_rows), block_rows))
        return carry

    def one_step(step, carry):
        gram_and_poly(x, gram, poly)

        @pl.when(step < NS_STEPS - 1)
        def _():
            lax.fori_loop(0, blocks, one_block, 0)
        return carry
    lax.fori_loop(0, NS_STEPS, one_step, 0)
    last_rows()


def muon_kernel(w1_ref, m1_ref, g1_ref, w2_ref, m2_ref, g2_ref,
                nw1, nm1, nw2, nm2,
                b1, b2, x1, x2, o1, o2, gram1, poly1, gram2, poly2, sq_out, sq_in,
                m_load, g_load, w_load, in_send, in_recv, sq_send, sq_recv, out_send, out_recv):
    data = lax.axis_index('data')
    model = lax.axis_index('model')
    core = lax.rem(data, 2)
    me = data * 4 + model
    rows = b1.shape[1]
    stacks = ((m1_ref, g1_ref, w1_ref, nw1, nm1, b1, x1, o1, b1.shape[2]),
              (m2_ref, g2_ref, w2_ref, nw2, nm2, b2, x2, o2, b2.shape[2]))

    def peer(slot):
        return xor2(data, lax.rem(slot, 4)), xor2(model, lax.div(slot, 4))

    def expert_of(slot):
        to_data, to_model = peer(slot)
        return to_data * 4 + to_model

    def loop(lo, hi, action):
        def body(i, carry):
            action(i)
            return carry
        lax.fori_loop(lo, hi, body, 0)

    inner = flip(lax.rem(model, 2), lax.div(model, 2))

    def slot_of(dz, dd):
        high = lax.div(dz, 2)
        if SWAP:
            dz = high * 2 + flip(lax.rem(dz, 2), high * inner)
        return dz * 4 + dd

    def slot_at(i):
        if DZ_FAST:
            return slot_of(lax.rem(i, 4), lax.div(i, 4))
        return slot_of(lax.div(i, 4), lax.rem(i, 4))

    def core_slots(target_core, action):
        low = flip(core, target_core)

        def at(j):
            if DZ_FAST:
                return slot_of(lax.rem(j + 2 * core, 4), lax.div(j, 4) * 2 + low)
            return slot_of(lax.div(j, 2), lax.rem(j, 2) * 2 + low)
        loop(0, 8, lambda j: action(at(j)))

    def row_slice(index):
        return pl.ds(pl.multiple_of(index * rows, rows), rows)

    def col_slice(index, cols):
        return pl.ds(pl.multiple_of(index * cols, cols), cols)

    def remote(source, target, send, recv, slot):
        to_data, to_model = peer(slot)
        return pltpu.make_async_remote_copy(
            src_ref=source, dst_ref=target, send_sem=send, recv_sem=recv,
            device_id={'data': to_data, 'model': to_model}, device_id_type=MESH)

    def load_m(which, slot):
        e = expert_of(slot)
        return pltpu.make_async_copy(stacks[which][0].at[e], stacks[which][4].at[e], m_load.at[which, slot])

    def load_g(which, slot):
        e = expert_of(slot)
        return pltpu.make_async_copy(stacks[which][1].at[e], stacks[which][5].at[e], g_load.at[which, slot])

    def load_w(which):
        return pltpu.make_async_copy(stacks[which][2], stacks[which][3], w_load.at[which])

    def copy_sq(which, slot):
        return remote(sq_out.at[which, slot], sq_in.at[which, slot],
                      sq_send.at[which, slot], sq_recv.at[which, slot], slot)

    def copy_in(which, slot):
        src, dst, cols = stacks[which][5], stacks[which][6], stacks[which][8]
        return remote(src.at[expert_of(slot)], dst.at[row_slice(data), col_slice(model, cols)],
                      in_send.at[which, slot], in_recv.at[which, slot], slot)

    def copy_out(which, slot):
        src, dst, cols = stacks[which][6], stacks[which][7], stacks[which][8]
        to_data, to_model = peer(slot)
        return remote(src.at[row_slice(to_data), col_slice(to_model, cols)], dst.at[me],
                      out_send.at[which, slot], out_recv.at[which, slot], slot)

    def momentum(which, slot):
        nm, blocks = stacks[which][4], stacks[which][5]
        e = expert_of(slot)
        load_m(which, slot).wait()
        load_g(which, slot).wait()
        mom = MOMENTUM * nm[e] + blocks[e].astype(F32)
        nm[e] = mom
        blocks[e] = mom.astype(BF16)
        sq_out[which, slot] = fold_squares(mom)

    def norm_of(which):
        loop(1, 16, lambda slot: copy_sq(which, slot).wait_recv())
        total = jnp.sum(sq_in[which], axis=0)
        return jnp.sqrt(jnp.sum(total, keepdims=True)) + NORM_EPS

    def receive(which):
        blocks, x, cols = stacks[which][5], stacks[which][6], stacks[which][8]
        sq_in[which, 0] = sq_out[which, 0]
        norm = norm_of(which)
        own = (row_slice(data), col_slice(model, cols))
        x[own] = (blocks[me].astype(F32) / norm).astype(BF16)

        def take(slot):
            copy_in(which, slot).wait_recv()
            from_data, from_model = peer(slot)
            at = (row_slice(from_data), col_slice(from_model, cols))
            x[at] = (x[at].astype(F32) / norm).astype(BF16)
        loop(1, 16, take)

    def weight_step(which, e, ortho):
        new_w, x, cols = stacks[which][3], stacks[which][6], stacks[which][8]
        scale = 0.2 * math.sqrt(max(x.shape[0], x.shape[1]))
        old = new_w[e]
        new_w[e] = old - LEARN_RATE * (ortho.astype(F32) * scale + DECAY * old)

    def own_step(which):
        x, cols = stacks[which][6], stacks[which][8]
        weight_step(which, me, x[row_slice(data), col_slice(model, cols)])

    def peer_step(which, slot):
        copy_out(which, slot).wait_recv()
        e = expert_of(slot)
        weight_step(which, e, stacks[which][7][e])

    for which in (1, 0):
        def load(slot):
            load_m(which, slot).start()
            load_g(which, slot).start()
        if which:
            loop(1, 16, lambda i: load(slot_at(i)))
            load(0)
        else:
            loop(0, 16, load)
    load_w(1).start()
    load_w(0).start()

    barrier = pltpu.get_barrier_semaphore()

    def greet(slot):
        to_data, to_model = peer(slot)
        pl.semaphore_signal(barrier, inc=1, device_id={'data': to_data, 'model': to_model}, device_id_type=MESH)
    loop(1, 16, greet)
    pl.semaphore_wait(barrier, 15)

    def send2(slot):
        copy_sq(1, slot).start()
        copy_in(1, slot).start()

    def first(i):
        momentum(1, slot_at(i))

        @pl.when(i > 1)
        def _():
            send2(slot_at(i - 1))
    loop(1, 16, first)
    momentum(1, 0)
    send2(slot_at(15))

    loop(0, 16, lambda i: momentum(0, 15 - i))
    loop(1, 16, lambda slot: copy_sq(0, slot).start())

    def send1(slot):
        @pl.when(slot > 0)
        def _():
            copy_in(0, slot).start()
    core_slots(0, send1)
    core_slots(1, send1)

    receive(1)

    def finish2():
        loop(0, 4, lambda i: update_rows(x2, poly2, row_slice(i)))
    newton_schulz(x2, gram2, poly2, rows, finish2)
    loop(1, 16, lambda i: copy_out(1, slot_at(i)).start())

    receive(0)
    def finish1():
        update_rows(x1, poly1, row_slice(xor2(data, 3)))

        def send_rows(dd):
            for dz in range(4):
                slot = slot_of(lax.rem(dz + 2 * core, 4), dd)

                @pl.when(slot > 0)
                def _():
                    copy_out(0, slot).start()

        def body(i):
            update_rows(x1, poly1, row_slice(xor2(data, 3 - i)))
            send_rows(4 - i)
        loop(1, 4, body)
        load_w(1).wait()
        own_step(1)
        send_rows(0)
    newton_schulz(x1, gram1, poly1, rows, finish1)

    load_w(0).wait()
    own_step(0)
    loop(1, 16, lambda slot: peer_step(1, slot))
    for which in (1, 0):
        def sent(slot):
            copy_in(which, slot).wait_send()
            copy_sq(which, slot).wait_send()
        loop(1, 16, sent)
    for target_core in (0, 1):
        def take(slot):
            @pl.when(slot > 0)
            def _():
                peer_step(0, slot)
        core_slots(target_core, take)
    for which in (1, 0):
        loop(1, 16, lambda slot: copy_out(which, slot).wait_send())


def store_kernel(*refs):
    sources, targets, sems = refs[:4], refs[4:8], refs[8]
    step = 2
    copies = []
    for which in range(4):
        for part in range(16 // step):
            at = pl.ds(part * step, step)
            copies.append(pltpu.make_async_copy(
                sources[which].at[at], targets[which].at[at], sems.at[which, part]))
    for copy in copies:
        copy.start()
    for copy in copies:
        copy.wait()


def store(arrays):
    return pl.pallas_call(
        store_kernel,
        out_shape=tuple(jax.ShapeDtypeStruct(a.shape, a.dtype) for a in arrays),
        in_specs=[pl.BlockSpec(memory_space=pltpu.VMEM)] * 4,
        out_specs=(pl.BlockSpec(memory_space=pl.ANY),) * 4,
        scratch_shapes=[pltpu.SemaphoreType.DMA((4, 8))],
        compiler_params=pltpu.CompilerParams(vmem_limit_bytes=1 << 20),
        name='store')(*(pltpu.with_memory_space_constraint(a, pltpu.VMEM) for a in arrays))


def solution(mesh):
    block_spec = P('stage', 'data', 'model')

    def local_step(w1, m1, g1, w2, m2, g2):
        experts, rows, cols1 = m1.shape
        cols2 = m2.shape[2]
        full_rows, size1, size2 = rows * 4, cols1 * 4, cols2 * 4
        dma = pltpu.SemaphoreType.DMA
        scratch = [pltpu.VMEM(g1.shape, BF16), pltpu.VMEM(g2.shape, BF16),
                   pltpu.VMEM((full_rows, size1), BF16), pltpu.VMEM((full_rows, size2), BF16),
                   pltpu.VMEM(g1.shape, BF16), pltpu.VMEM(g2.shape, BF16),
                   pltpu.VMEM((size1, size1), BF16), pltpu.VMEM((size1, size1), BF16),
                   pltpu.VMEM((size2, size2), BF16), pltpu.VMEM((size2, size2), BF16),
                   pltpu.VMEM((2, 16, 8, 128), F32), pltpu.VMEM((2, 16, 8, 128), F32),
                   dma((2, 16)), dma((2, 16)), dma((2,))] + [dma((2, 16))] * 6
        return store(pl.pallas_call(
            muon_kernel,
            out_shape=tuple(pltpu.VMEM(a.shape, F32) for a in (w1, m1, w2, m2)),
            in_specs=[pl.BlockSpec(memory_space=pl.ANY)] * 6,
            out_specs=(pl.BlockSpec(memory_space=pltpu.VMEM),) * 4,
            scratch_shapes=scratch,
            compiler_params=pltpu.CompilerParams(
                collective_id=0, has_side_effects=True, vmem_limit_bytes=36 << 20),
            name='muon')(w1, m1, g1, w2, m2, g2))

    return jax.shard_map(local_step, mesh=mesh, in_specs=(block_spec,) * 6, out_specs=(block_spec,) * 4, check_vma=False)
```
